32 devices in a mesh: blk: 8 (over y, x, core), heads: 4 (over z).
Axes of the slice: x: 2, y: 2, z: 4, core: 2. Of those that a mesh axis runs over, the one named last changes fastest.
Arguments:
- queries: bfloat16 [2048, 4096], P('blk', 'heads'), may hold values from -5 to 5
- keys: bfloat16 [2048, 1024], P('blk', 'heads'), may hold values from -5 to 5
- values: bfloat16 [2048, 1024], P('blk', 'heads'), may hold values from -6 to 6
- doc_ids: int32 [2048], P('blk'), may hold values from 0 to 7, never falling along the last dimension, each value on 1 to 1024 neighbouring positions
Outputs:
- attended: bfloat16 [2048, 4096], P('blk', 'heads')
The draws below stay inside these ranges and needn't reach their ends.
Inputs may be any that keep to these rules, and one draw needn't show every extreme that they name: `doc_ids`: Non-decreasing along the sequence; every document has 1024 tokens at most, and some document exactly 1024.
All inputs are finite; a program needn't handle non-finite values.
Results may differ from the reference program's by a relative error of at most 0.0034.
Values may be sent and summed in bfloat16 or wider, within the bound.
A program may use at most 64 MiB of HBM per device.

```python
import math
import jax
import jax.numpy as jnp
import numpy as np
from jax import lax

QUERY_HEAD_COUNT = 32
KEY_VALUE_HEADS = 8
HEAD_WIDTH = 128
BLOCK_TOKENS = 256
DOC_BLKS = 4
MAXDOC = 1024
PACKED_TOKENS = 2048
DOCS = 8


def make_pair(key):
    start_offset = jax.random.fold_in(key, 7)
    key_portion = jnp.clip(jax.random.normal(jax.random.fold_in(start_offset, 1), (PACKED_TOKENS, KEY_VALUE_HEADS * HEAD_WIDTH), jnp.float32), -4.0, 4.0)
    query_part = jnp.clip(jax.random.normal(jax.random.fold_in(start_offset, 2), (PACKED_TOKENS, QUERY_HEAD_COUNT * HEAD_WIDTH), jnp.float32), -4.0, 4.0)
    return (query_part, key_portion)


def draw_queries(key, part):
    return make_pair(key)[0].astype(jnp.bfloat16)


def draw_keys(key, part):
    return make_pair(key)[1].astype(jnp.bfloat16)


def block_levels(own_key, shape, cuts, smallest, high):
    loudness = 1.0
    for dim, parts in cuts:
        draws = jax.random.uniform(jax.random.fold_in(jax.random.fold_in(own_key, 6), dim), (parts,), jnp.float32, smallest / len(cuts), high / len(cuts))
        loudness = loudness * jnp.repeat(jnp.exp(draws), shape[dim] // parts).reshape((-1,) + (1,) * (len(shape) - 1 - dim))
    return loudness


def profile(count, total, limit, slope):
    loads = [(1 << 20) // math.isqrt(standing ** slope) + 1 for standing in range(2, count + 1)]
    surplus, counts = total - limit - (count - 1), [1] * (count - 1)
    while surplus > 0:
        movable = [i for i in range(count - 1) if counts[i] < limit]
        whole, left = sum([loads[i] for i in movable]), surplus
        for i in movable:
            addition = min(limit - counts[i], max(1, left * loads[i] // whole), surplus)
            counts[i] = counts[i] + addition
            surplus = surplus - addition
    return np.array([limit] + counts)


def ragged_sizes(stream_key, count, total, most, slope):
    if count == 2:
        one = jax.random.randint(stream_key, (), max(1, total - most), min(most, total - 1) + 1)
        return jnp.stack([one, total - one])
    sizes = jnp.asarray(profile(count, total, most, slope), jnp.int32)
    twos = (count - 1) // 2
    source_of, taker = sizes[1:1 + 2 * twos:2], sizes[2:2 + 2 * twos:2]
    room = jnp.minimum(source_of - 1, most - taker)
    shifted = jax.random.randint(jax.random.fold_in(stream_key, 1), (twos,), 0, 1 << 20) % (room + 1)
    sizes = sizes.at[1:1 + 2 * twos:2].set(source_of - shifted).at[2:2 + 2 * twos:2].set(taker + shifted)
    return sizes[jax.random.permutation(jax.random.fold_in(stream_key, 2), count)]


def gaussian(own_key, dims, spread, most, split=(), held_as=jnp.bfloat16):
    array = jax.random.normal(own_key, dims, jnp.float32) * spread
    if len(split) > 0:
        array = block_levels(own_key, dims, split, -0.22, 0.18) * array
    return jnp.clip(array, min=-most, max=most).astype(held_as)


def setup_inputs(seed: int = 0) -> dict:
    arg_keys = jax.random.split(jax.random.key(seed), 5)
    return {
        "queries": draw_queries(jax.random.fold_in(arg_keys[4], 71), 0),
        "keys": draw_keys(jax.random.fold_in(arg_keys[4], 71), 0),
        "values": gaussian(arg_keys[2], (PACKED_TOKENS, KEY_VALUE_HEADS * HEAD_WIDTH), 1.0, 6.0, ((0, 8), (1, 4))),
        "doc_ids": jnp.searchsorted(jnp.cumsum(ragged_sizes(arg_keys[3], DOCS, PACKED_TOKENS, MAXDOC, 2)), jnp.arange(PACKED_TOKENS), side="right").astype(jnp.int32),
    }


def reference(queries, keys, values, doc_ids):
    seq_length = queries.shape[0]
    backward_extent = DOC_BLKS * BLOCK_TOKENS
    visible_span = backward_extent + BLOCK_TOKENS
    queries_per_group = QUERY_HEAD_COUNT // KEY_VALUE_HEADS
    score_scale = 1.0 / math.sqrt(HEAD_WIDTH)
    padded_key_rows = jnp.concatenate([jnp.zeros((backward_extent, KEY_VALUE_HEADS * HEAD_WIDTH), keys.dtype), keys], axis=0)
    padded_value_rows = jnp.concatenate([jnp.zeros((backward_extent, KEY_VALUE_HEADS * HEAD_WIDTH), values.dtype), values], axis=0)
    docs_padded = jnp.concatenate([-jnp.ones((backward_extent,), jnp.int32), doc_ids.astype(jnp.int32)], axis=0)

    def one_block(block_index):
        first_row = (block_index * BLOCK_TOKENS).astype(jnp.int32)
        block_of_queries = lax.dynamic_slice_in_dim(queries, first_row, BLOCK_TOKENS, 0)
        block_of_queries = block_of_queries.reshape(BLOCK_TOKENS, KEY_VALUE_HEADS, queries_per_group, HEAD_WIDTH).astype(jnp.float32)
        block_of_keys = lax.dynamic_slice_in_dim(padded_key_rows, first_row, visible_span, 0)
        block_of_keys = block_of_keys.reshape(visible_span, KEY_VALUE_HEADS, HEAD_WIDTH).astype(jnp.float32)
        block_of_values = lax.dynamic_slice_in_dim(padded_value_rows, first_row, visible_span, 0)
        block_of_values = block_of_values.reshape(visible_span, KEY_VALUE_HEADS, HEAD_WIDTH).astype(jnp.float32)
        query_docs = lax.dynamic_slice_in_dim(doc_ids.astype(jnp.int32), first_row, BLOCK_TOKENS, 0)
        key_docs = lax.dynamic_slice_in_dim(docs_padded, first_row, visible_span, 0)
        query_pos = first_row + jnp.arange(BLOCK_TOKENS, dtype=jnp.int32)
        key_pos = first_row - backward_extent + jnp.arange(visible_span, dtype=jnp.int32)
        allowed = (query_docs[:, None] == key_docs[None, :]) & (key_pos[None, :] <= query_pos[:, None])
        scores = jnp.einsum('qkgd,skd->kgqs', block_of_queries, block_of_keys) * score_scale
        scores = jnp.where(allowed, scores, -jnp.inf)
        rowmax = lax.optimization_barrier(jnp.max(scores, axis=-1, keepdims=True))
        weights = jnp.exp(scores - rowmax)
        denominator = lax.optimization_barrier(jnp.sum(weights, axis=-1))
        rounded = lax.optimization_barrier(weights.astype(jnp.bfloat16)).astype(jnp.float32)
        numerator = jnp.einsum('kgqs,skd->qkgd', rounded, block_of_values)
        result = numerator / jnp.transpose(denominator, (2, 0, 1))[..., None]
        return result.reshape(BLOCK_TOKENS, QUERY_HEAD_COUNT * HEAD_WIDTH).astype(jnp.bfloat16)
    blocks_out = lax.map(one_block, jnp.arange(seq_length // BLOCK_TOKENS, dtype=jnp.int32))
    return blocks_out.reshape(seq_length, QUERY_HEAD_COUNT * HEAD_WIDTH)
```

```python
import functools
import math

import jax
import jax.numpy as jnp
from jax import lax
from jax.experimental import pallas as pl
from jax.experimental.pallas import tpu as pltpu
from jax.sharding import PartitionSpec as P

HEAD_WIDTH = 128
DOC_BLKS = 4
MESH = pl.DeviceIdType.MESH
NEG = -1e30
S_SLOTS = 2
P_SLOTS = 4
scope = jax.named_scope


def fold(x, op, chains=4):
    parts = jnp.split(x, chains, axis=0)
    while len(parts) > 1:
        parts = [op(a, b) for a, b in zip(parts[::2], parts[1::2])]
    return parts[0]


def kernel(n, q_hbm, k_hbm, v_hbm, doc_hbm, o_ref,
           qbuf, qt, kv, docs, bias, mref, lref, acc, sbuf, mbuf, pbuf, abuf,
           qsem, loadsem, docsem, docsend, docrecv, send, recv):
    rows = q_hbm.shape[0]
    kv_heads = k_hbm.shape[1] // HEAD_WIDTH
    heads = q_hbm.shape[1] // HEAD_WIDTH
    group = heads // kv_heads
    chunks = 2 * kv_heads
    scale = math.log2(math.e) / math.sqrt(HEAD_WIDTH)

    me = lax.axis_index("blk")
    core = lax.rem(me, 2)
    pair = me // 2
    pairs = n // 2

    def columns(h):
        return slice(h * HEAD_WIDTH, (h + 1) * HEAD_WIDTH)

    load_q = pltpu.make_async_copy(q_hbm, qbuf, qsem)
    load_doc = pltpu.make_async_copy(doc_hbm, docs.at[0], docsem)
    for i in range(chunks):
        src = (k_hbm, v_hbm)[i % 2].at[:, pl.ds((i // 2) * HEAD_WIDTH, HEAD_WIDTH)]
        pltpu.make_async_copy(src, kv.at[0, i], loadsem).start()
    load_doc.start()
    load_q.start()

    far = me + 4 < n
    relayed_source = (lax.rem(pair, 4) == 1) & (pair + 2 < pairs)
    skips = (me + 2 < n) & relayed_source
    near = (me + 2 < n) & jnp.logical_not(relayed_source)
    late = (lax.rem(pair, 4) == 2) & (pair + 1 < pairs)
    has4 = me >= 4
    has2 = me >= 2
    relays = has4 & (lax.rem(pair, 4) == 3)

    barrier = pltpu.get_barrier_semaphore()

    def greet(cond, step):
        @pl.when(cond)
        def _():
            pl.semaphore_signal(barrier, inc=1, device_id={"blk": me + step}, device_id_type=MESH)

    for o in range(1, DOC_BLKS + 1):
        greet(me >= o, -o)
    greet(core == 0, 1)
    greet(late, 2)
    with scope("barrier"):
        pl.semaphore_wait(barrier, jnp.minimum(n - 1 - me, DOC_BLKS) + core + relays.astype(jnp.int32))

    def doc_copy(o):
        return pltpu.make_async_remote_copy(
            src_ref=docs.at[0], dst_ref=docs.at[o], send_sem=docsend.at[o - 1], recv_sem=docrecv.at[o - 1],
            device_id={"blk": me + o}, device_id_type=MESH)

    FAR, NEAR, OWN, BACK, FOUR, TWO = range(6)
    half = rows // 2
    K0, V0, K1, V1 = range(4)

    def piece(slot, i, part):
        if part is None:
            return kv.at[slot, i]
        return kv.at[slot, i, pl.ds(part * half, half)]

    def arrival(slot, i, part):
        base = {4: 0, 2: 2 * chunks, 3: 4 * chunks, 1: 5 * chunks}
        if slot in (4, 2):
            return recv.at[base[slot] + 2 * i + (part or 0)]
        return recv.at[base[slot] + i]

    def copy(flow, i, part=None):
        if flow == TWO:
            src, dst, step = 2, jnp.where(core == 0, 3, 1), 1 - 2 * core
            sem = recv.at[jnp.where(core == 0, 4 * chunks, 5 * chunks) + i]
        else:
            src, dst, step = {FAR: (0, 4, 4), NEAR: (0, 2, 2), OWN: (0, 1, 1), BACK: (4, 2, -2), FOUR: (4, 3, -1)}[flow]
            sem = arrival(dst, i, part)
        return pltpu.make_async_remote_copy(
            src_ref=piece(src, i, part), dst_ref=piece(dst, i, part),
            send_sem=send.at[flow], recv_sem=sem,
            device_id={"blk": me + step}, device_id_type=MESH)

    def push(cond, flow, i, part=None):
        @pl.when(cond)
        def _():
            copy(flow, i, part).start()

    def arrived(slot, i, part=None):
        pltpu.make_async_remote_copy(
            src_ref=piece(0, i, part), dst_ref=piece(slot, i, part), send_sem=send.at[OWN],
            recv_sem=arrival(slot, i, part),
            device_id={"blk": lax.rem(me + 1, n)}, device_id_type=MESH).wait_recv()

    load_doc.wait()
    for o in range(1, DOC_BLKS + 1):
        @pl.when(me + o < n)
        def _():
            doc_copy(o).start()

    with scope("ld"):
        pltpu.make_async_copy(kv.at[1], kv.at[0], loadsem).wait()
    third = jnp.where(relayed_source, V1, K1)
    fourth = jnp.where(relayed_source, K1, V1)
    for i in (K0, V0, third, fourth):
        for part in range(2):
            push(far, FAR, i, part)
        push(near, NEAR, i)
        if i is K0 or i is V0:
            push(core == 0, OWN, i)
    push(core == 0, OWN, K1)
    push(core == 0, OWN, V1)
    push(skips, NEAR, K1)

    def column(row):
        return jnp.broadcast_to(row, (HEAD_WIDTH, rows)).T

    def make_bias(o):
        key_docs = column(docs[o, 0:1, :])
        for c in range(rows // HEAD_WIDTH):
            cols = columns(c)
            ok = key_docs == docs[0, 0:1, cols]
            if isinstance(o, int) and o == 0:
                s = lax.broadcasted_iota(jnp.int32, (rows, HEAD_WIDTH), 0)
                r = lax.broadcasted_iota(jnp.int32, (rows, HEAD_WIDTH), 1) + c * HEAD_WIDTH
                ok = ok & (s <= r)
            bias[o, :, cols] = jnp.where(ok, 0.0, NEG)

    def scores(o, h):
        k = kv[o, 2 * (h // group)]
        s = jnp.dot(jnp.concatenate([k, k], axis=1), qt[h], preferred_element_type=jnp.float32) + bias[o]
        return s, jnp.max(fold(s, jnp.maximum), axis=0, keepdims=True)

    def weigh(o, h, s, m):
        alpha = None
        if o != 0:
            old = mref[h]
            m = jnp.maximum(m, old)
            alpha = jnp.exp2(old - m)
        w = jnp.exp2(s - m)
        l = jnp.sum(fold(w, jnp.add), axis=0, keepdims=True)
        if o != 0:
            l = l + lref[h] * alpha
        mref[h] = m
        lref[h] = l
        return w.astype(jnp.bfloat16), alpha

    def gather(o, h, w, alpha, values_t):
        a = jnp.dot(values_t, w, preferred_element_type=jnp.float32)
        acc[h] = a if o == 0 else a + acc[h] * alpha

    def attend(o, batch=2):
        values_t = {}
        scored, weighed = {}, {}
        for t in range(0, heads + 2 * batch, batch):
            for h in range(t, t + batch):
                if h < heads:
                    scored[h] = scores(o, h)
                h -= 2 * batch
                if h >= 0:
                    g = h // group
                    if g not in values_t:
                        values_t[g] = kv[o, 2 * g + 1].T
                    gather(o, h, *weighed.pop(h), values_t[g])
                h += batch
                if 0 <= h < heads:
                    weighed[h] = weigh(o, h, *scored.pop(h))

    def do(A=(), B=(), C=(), fin=()):
        name = "".join("A%d%d" % t for t in A) + "".join("B%d%d" % t for t in B) + "".join("C%d%d" % t for t in C)
        with scope(name):
            values_t = {t: kv[t[0], 2 * t[1] + 1].T for t in C}
            for j in range(group):
                for t in A:
                    s, m = scores(t[0], t[1] * group + j)
                    sbuf[s_slot[t], j] = s
                    mbuf[s_slot[t], j] = m
                for t in C:
                    w = p_slot[t]
                    gather(t[0], t[1] * group + j, pbuf[w, j], abuf[w, j], values_t[t])
                for t in B:
                    x = s_slot[t]
                    w, alpha = weigh(t[0], t[1] * group + j, sbuf[x, j], mbuf[x, j])
                    pbuf[p_slot[t], j] = w
                    abuf[p_slot[t], j] = alpha
            for g in fin:
                finish(g)

    def finish(g):
        for h in range(g * group, (g + 1) * group):
            o_ref[:, columns(h)] = (acc[h] / lref[h]).T.astype(o_ref.dtype)

    s_slot, p_slot = {}, {}

    def plan(steps):
        s_slot.clear()
        p_slot.clear()
        free_s, free_p = list(range(S_SLOTS)), list(range(P_SLOTS))
        for step in steps:
            for t in step.get("B", ()):
                p_slot[t] = free_p.pop(0)
            for t in step.get("A", ()):
                s_slot[t] = free_s.pop(0)
            free_s += [s_slot[t] for t in step.get("B", ())]
            free_p += [p_slot[t] for t in step.get("C", ())]

    def receive(event):
        kind, i = event[0], event[1]
        part = event[2] if len(event) > 2 else None
        with scope("w" + "".join(str(e) for e in event)):
            arrived(kind, i, part)
        if kind == 4:
            if i != K1 and part is not None:
                push(relays, BACK, i, part)

    def run(steps):
        plan(steps)
        for step in steps:
            for event in step.get("W", ()):
                if event[0] == "f4":
                    push(core == 1, FOUR, event[1])
                elif event[0] == "f2":
                    copy(TWO, event[1]).start()
                else:
                    receive(event)
            rest = {k: v for k, v in step.items() if k != "W"}
            if rest:
                do(**rest)

    with scope("ldq"):
        load_q.wait()
    with scope("prep"):
        for h in range(heads):
            x = qbuf[:, columns(h)].T.astype(jnp.float32) * scale
            hi = x.astype(jnp.bfloat16)
            qt[h, :HEAD_WIDTH] = hi
            qt[h, HEAD_WIDTH:] = (x - hi.astype(jnp.float32)).astype(jnp.bfloat16)
        make_bias(0)
    with scope("own"):
        attend(0)

    def receive_docs(o):
        @pl.when(me >= o)
        def _():
            doc_copy(o).wait_recv()
            make_bias(o)

    with scope("docs1"):
        receive_docs(1)

    @pl.when(core == 1)
    def _():
        with scope("w1"):
            for i in range(chunks):
                arrived(1, i)
        with scope("a1"):
            attend(1)

    with scope("docs"):
        for o in range(2, DOC_BLKS + 1):
            receive_docs(o)

    def role(cond, steps):
        @pl.when(cond)
        def _():
            run(steps)

    def w4(i):
        return [(4, i, 0), (4, i, 1), ("f4", i)]

    def w2(i):
        return [(2, i), ("f2", i)]

    def w2r(i):
        return [(2, i, 0), (2, i, 1), ("f2", i)]

    t = lambda *names: [(int(x[0]), int(x[1])) for x in names]
    S = lambda W=(), A=(), B=(), C=(), fin=(): {k: v for k, v in dict(W=list(W), A=t(*A), B=t(*B), C=t(*C), fin=fin).items() if v}

    role(has4 & late & (core == 0), [
        S(w4(K0), ["40"]),
        S([(3, K0)], ["30"], ["40"]),
        S(w4(V0), [], ["30"], ["40"]),
        S([(3, V0)], [], [], ["30"]),
        S(w2r(K0), ["20"]),
        S(w4(K1), ["41"], ["20"]),
        S(w2(K1) + [(1, K0)], ["10"], ["41"]),
        S([], ["21"], ["10"]),
        S(w2r(V0) + [(3, K1)], ["31"], ["21"], ["20"]),
        S([(1, K1), (1, V0)], ["11"], ["31"], ["10"]),
        S(w4(V1) + w2r(V1), [], ["11"], ["41", "21"], [0]),
        S([(3, V1), (1, V1)], [], [], ["31", "11"], [1]),
    ])
    role(has4 & late & (core == 1), [
        S(w4(K0), ["40"]),
        S(w4(V0), [], ["40"], ["40"]) if False else S([], [], ["40"]),
        S(w4(V0), [], [], ["40"]),
        S(w2r(K0), ["20"]),
        S(w4(K1), ["41"], ["20"]),
        S(w2(K1) + [(3, K0)], ["30"], ["41"]),
        S([], ["21"], ["30"]),
        S(w2r(V0), [], ["21"], ["20"]),
        S([(3, K1), (3, V0)], ["31"], [], ["30"]),
        S(w4(V1) + w2r(V1), [], ["31"], ["41", "21"], [0]),
        S([(3, V1)], [], [], ["31"], [1]),
    ])
    role(has4 & jnp.logical_not(late) & (core == 0), [
        S(w4(K0) + w2(K0), ["40"]),
        S([], ["20"], ["40"]),
        S([(4, V0, 0), (3, K0)], ["30"], ["20"]),
        S([(4, V0, 1), ("f4", V0)] + w2(V0) + [(1, K0)], ["10"], ["30"], ["40"]),
        S([(4, V1, 0)], [], ["10"], ["20"]),
        S([(4, V1, 1), ("f4", V1), (3, V0), (1, V0)], [], [], ["30", "10"], [0]),
        S(w2(K1), ["21"]),
        S(w4(K1), ["41"], ["21"]),
        S(w2(V1) + [(1, K1)], ["11"], ["41"], ["21"]),
        S([(3, K1)], ["31"], ["11"], ["41"]),
        S([(1, V1)], [], ["31"], ["11"]),
        S([(3, V1)], [], [], ["31"], [1]),
    ])
    role(has4 & jnp.logical_not(late) & (core == 1), [
        S(w4(K0) + w2(K0), ["40"]),
        S([], ["20"], ["40"]),
        S([(4, V0, 0), (3, K0)], ["30"], ["20"]),
        S([(4, V0, 1), ("f4", V0)] + w2(V0), [], ["30"], ["40", "20"]),
        S([(4, V1, 0)]),
        S([(4, V1, 1), ("f4", V1), (3, V0)], [], [], ["30"], [0]),
        S(w2(K1), ["21"]),
        S(w4(K1), ["41"], ["21"]),
        S(w2(V1) + [(3, K1)], ["31"], ["41"], ["21"]),
        S([], [], ["31"], ["41"]),
        S([(3, V1)], [], [], ["31"], [1]),
    ])
    for c, a in ((0, "1"), (1, "3")):
        b = int(a)
        role(has2 & jnp.logical_not(has4) & (core == c), [
            S(w2(K0), ["20"]),
            S([(b, K0)], [a + "0"], ["20"]),
            S(w2(V0), [], [a + "0"], ["20"]),
            S([(b, V0)], [], [], [a + "0"], [0]),
            S(w2(K1), ["21"]),
            S([(b, K1)], [a + "1"], ["21"]),
            S(w2(V1), [], [a + "1"], ["21"]),
            S([(b, V1)], [], [], [a + "1"], [1]),
        ])

    @pl.when(me < 2)
    def _():
        for g in range(kv_heads):
            finish(g)

    with scope("end"):
        for o in range(1, DOC_BLKS + 1):
            @pl.when(me + o < n)
            def _():
                doc_copy(o).wait_send()

        def sent(cond, flow, i):
            @pl.when(cond)
            def _():
                pltpu.make_async_remote_copy(
                    src_ref=kv.at[0, i], dst_ref=kv.at[1, i], send_sem=send.at[flow], recv_sem=recv.at[0],
                    device_id={"blk": lax.rem(me + 1, n)}, device_id_type=MESH).wait_send()

        full = slice(None)
        sent(skips, NEAR, K1)
        sent(near, NEAR, full)
        sent(far, FAR, full)
        sent(core == 0, OWN, full)
        sent(relays, BACK, pl.ds(0, chunks - 1))
        sent(has4 & (core == 1), FOUR, full)
        sent(has2, TWO, full)


def shards(n, queries, keys, values, doc_ids):
    rows = queries.shape[0]
    heads = queries.shape[1] // HEAD_WIDTH
    chunks = 2 * (keys.shape[1] // HEAD_WIDTH)
    group = heads * HEAD_WIDTH // keys.shape[1]
    slots = DOC_BLKS + 1
    hbm_spec = pl.BlockSpec(memory_space=pltpu.HBM)
    stat = pltpu.VMEM((heads, 1, rows), jnp.float32)
    return pl.pallas_call(
        functools.partial(kernel, n),
        out_shape=pltpu.VMEM(queries.shape, jnp.bfloat16),
        in_specs=[hbm_spec] * 4,
        out_specs=pl.BlockSpec(memory_space=pltpu.VMEM),
        scratch_shapes=[
            pltpu.VMEM(queries.shape, jnp.bfloat16),
            pltpu.VMEM((heads, 2 * HEAD_WIDTH, rows), jnp.bfloat16),
            pltpu.VMEM((slots, chunks, rows, HEAD_WIDTH), jnp.bfloat16),
            pltpu.VMEM((slots, 1, rows), jnp.int32),
            pltpu.VMEM((slots, rows, rows), jnp.float32),
            stat, stat,
            pltpu.VMEM((heads, HEAD_WIDTH, rows), jnp.float32),
            pltpu.VMEM((S_SLOTS, group, rows, rows), jnp.float32),
            pltpu.VMEM((S_SLOTS, group, 1, rows), jnp.float32),
            pltpu.VMEM((P_SLOTS, group, rows, rows), jnp.bfloat16),
            pltpu.VMEM((P_SLOTS, group, 1, rows), jnp.float32),
            pltpu.SemaphoreType.DMA,
            pltpu.SemaphoreType.DMA,
            pltpu.SemaphoreType.DMA,
            pltpu.SemaphoreType.DMA((DOC_BLKS,)),
            pltpu.SemaphoreType.DMA((DOC_BLKS,)),
            pltpu.SemaphoreType.DMA((6,)),
            pltpu.SemaphoreType.DMA((6 * chunks,)),
        ],
        compiler_params=pltpu.CompilerParams(collective_id=0, has_side_effects=True,
                                             vmem_limit_bytes=32 * 2**20),
    )(*(pltpu.with_memory_space_constraint(x, pltpu.HBM) for x in (queries, keys, values, doc_ids.reshape(1, rows))))


def solution(mesh):
    return jax.shard_map(
        functools.partial(shards, mesh.shape["blk"]),
        mesh=mesh,
        in_specs=(P("blk", "heads"), P("blk", "heads"), P("blk", "heads"), P("blk")),
        out_specs=P("blk", "heads"),
        check_vma=False,
    )
```
